32 devices in a mesh: row: 2 (over x), col: 16 (over z, y, core).
Axes of the slice: x: 2, y: 2, z: 4, core: 2. Of those that a mesh axis runs over, the one named last changes fastest.
Arguments:
- matrix: bfloat16 [1024, 65536], P('row', 'col'), may hold values from -0.1875 to 0.1875
- measured: float32 [256, 1024], P(None, 'row'), may hold values from -160 to 160
- support: int32 [4, 1024], replicated, may hold values from 0 to 65535, as said below
Outputs:
- estimate: float32 [256, 65536], P('row', 'col')
- row_norms: float32 [65536], P('col')
- residual_energy: float32 [4], replicated
The draws below stay inside these ranges and needn't reach their ends.
Inputs may be any that keep to these rules, and one draw needn't show every extreme that they name: Each row of support lists 1024 distinct signal-row indices in increasing order; in every row, each aligned block of 4096 indices (the signal rows of one index of col) holds at most 128 of them, and some block exactly 128.
All inputs are finite; a program needn't handle non-finite values.
Results may differ from the reference program's by a relative error of at most 0.015.
Values may be sent and summed in bfloat16 or wider, within the bound.
A program may use at most 64 MiB of HBM per device.

```python
import math
import jax
import jax.numpy as jnp
from jax import lax

MB = 512
NB = 4096
L = 256
KB = 64
ITERS = 4
M = 1024
N = 65536
K = 1024
N_ROW = 2
N_COL = 16


def draw_measured(key, part):
    key_base, key_rows, key_signals = jax.random.split(key, 3)
    position = jnp.arange(M, dtype=jnp.float32) / max(M - 1, 1)
    rising = math.log(3.0)
    values = jax.random.normal(key_base, (L, M), jnp.float32)
    values = jnp.clip(values, -5.0, 5.0)
    row_scale = jnp.exp(rising * position + jax.random.uniform(key_rows, (M,), jnp.float32) * math.log(10.0 / 3.0)) / 3.0
    signal_scale = jnp.exp(jax.random.uniform(key_signals, (L,), jnp.float32) * math.log(10.0)) / math.sqrt(10.0)
    return values * row_scale[None, :] * signal_scale[:, None]


def draw_support(key, part):
    blocks = N // NB

    def one_iteration(iteration_key):
        key_order, key_shift, key_ranks = jax.random.split(iteration_key, 3)
        block_order = jax.random.permutation(key_order, blocks)
        shifts = jax.random.randint(key_shift, (blocks // 2,), 0, KB + 1).at[0].set(KB)
        counts = jnp.zeros((blocks,), jnp.int32).at[block_order[0::2]].set(KB + shifts).at[block_order[1::2]].set(KB - shifts)
        rank_table = jax.vmap(lambda block_key: jax.random.permutation(block_key, NB))(jax.random.split(key_ranks, blocks))
        chosen = (rank_table < counts[:, None]).reshape(-1)
        return jnp.nonzero(chosen, size=K)[0].astype(jnp.int32)
    return jax.vmap(one_iteration)(jax.random.split(key, ITERS))


def shard_levels(key, extent, cuts, least, largest):
    factor_of = 1.0
    for dim, shards_of in cuts:
        steps = jax.random.uniform(jax.random.fold_in(jax.random.fold_in(key, 6), dim), (shards_of,), jnp.float32, least / len(cuts), largest / len(cuts))
        factor_of = factor_of * jnp.repeat(jnp.exp(steps), extent[dim] // shards_of).reshape((-1,) + (1,) * (len(extent) - 1 - dim))
    return factor_of


def scatter_about(own_key, extent, deviation, bound, cuts=(), kind=jnp.bfloat16):
    result = deviation * jax.random.normal(own_key, extent, jnp.float32)
    if cuts:
        result = result * shard_levels(own_key, extent, cuts, -0.22, 0.18)
    return jnp.clip(result, -bound, bound).astype(kind)


def setup_inputs(seed: int = 0) -> dict:
    key_of = jax.random.split(jax.random.key(seed), 4)
    return {
        "matrix": scatter_about(key_of[0], (M, N), M ** -0.5, 0.1875, ((0, 2), (1, 16))),
        "measured": draw_measured(jax.random.fold_in(key_of[3], 71), 0),
        "support": draw_support(jax.random.fold_in(key_of[3], 71), 0),
    }


STEP_SIZE = 0.25

def predict(matrix, current_half):

    def add_block(block, summed):
        start_col = (block * NB).astype(jnp.int32)
        columns = lax.dynamic_slice_in_dim(matrix, start_col, NB, 1)
        signal_cols = lax.dynamic_slice_in_dim(current_half, start_col, NB, 1)
        return summed + lax.dot_general(signal_cols, columns, (((1,), (1,)), ((), ())), preferred_element_type=jnp.float32)
    return lax.fori_loop(0, N_COL, add_block, jnp.zeros((L, MB * N_ROW), jnp.float32))

def descend(matrix, residual_half):

    def one_block(block):
        start_col = (block * NB).astype(jnp.int32)
        columns = lax.dynamic_slice_in_dim(matrix, start_col, NB, 1)
        summed = jnp.zeros((L, NB), jnp.float32)
        for group_index in range(N_ROW):
            part_sum = jnp.dot(residual_half[:, group_index * MB:(group_index + 1) * MB], columns[group_index * MB:(group_index + 1) * MB], preferred_element_type=jnp.float32)
            rounded = lax.optimization_barrier(part_sum.astype(jnp.bfloat16))
            summed = summed + rounded.astype(jnp.float32)
        return summed
    blocks_out = lax.map(one_block, jnp.arange(N_COL, dtype=jnp.int32))
    return jnp.transpose(blocks_out, (1, 0, 2)).reshape(L, N_COL * NB)

def reference(matrix, measured, support):
    total_cols = NB * N_COL
    current = jnp.zeros((L, total_cols), jnp.float32)
    energies = []
    stepped = current
    for iteration in range(ITERS):
        if iteration == 0:
            residual = measured
        else:
            residual = measured - predict(matrix, current.astype(jnp.bfloat16))
        energies.append(jnp.sum(residual * residual) / (L * MB * N_ROW))
        gradient = descend(matrix, residual.astype(jnp.bfloat16))
        stepped = current + STEP_SIZE * gradient
        keep_mask = jnp.zeros((total_cols,), jnp.float32).at[support[iteration]].set(1.0)
        current = stepped * keep_mask[None, :]
    row_norms = jnp.sqrt(lax.optimization_barrier(jnp.sum(stepped * stepped, axis=0)))
    return (current, row_norms, jnp.stack(energies))
```

```python
import jax
import jax.numpy as jnp
from jax import lax
from jax.sharding import PartitionSpec as P

KMAX = 128
STEP_SIZE = 0.25
HI = lax.Precision.HIGHEST
NT = (((1,), (1,)), ((), ()))


def window(support_row, start, width):
    below = jnp.sum((support_row < start).astype(jnp.int32))
    local = support_row - start
    inside = (local >= 0) & (local < width)
    slot = jnp.arange(support_row.shape[0]) - below
    chosen = (slot[None, :] == jnp.arange(KMAX)[:, None]) & inside[None, :]
    return jnp.sum(jnp.where(chosen, local[None, :] + 1, 0), axis=1) - 1


def local(matrix, measured, support):
    signals = measured.shape[0]
    n_row = lax.axis_size("row")
    rows_mine = signals // n_row
    columns = matrix.shape[1]
    offset = lax.axis_index("col") * columns
    iterations = support.shape[0]
    total_count = signals * measured.shape[1] * n_row
    lanes = jnp.arange(columns)
    index = [window(support[t], offset, columns) for t in range(iterations)]
    onehot = [(i[:, None] == lanes[None, :]).astype(jnp.bfloat16) for i in index]
    kept = [
        lax.dot_general(e, matrix, NT, preferred_element_type=jnp.float32).astype(jnp.bfloat16)
        for e in onehot[:-1]
    ]
    residual = measured
    current = jnp.zeros((signals, KMAX), jnp.float32)
    energies = []
    for t in range(iterations):
        energies.append(jnp.sum(residual * residual))
        half = residual.astype(jnp.bfloat16)
        if t == iterations - 1:
            break
        part = lax.dot_general(half, kept[t], NT, preferred_element_type=jnp.float32)
        gradient = lax.psum(part.astype(jnp.bfloat16), "row").astype(jnp.float32)
        if t:
            same = (index[t - 1][:, None] == index[t][None, :]) & (index[t] >= 0)[None, :]
            current = jnp.dot(current, same.astype(jnp.float32), precision=HI)
        current = current + STEP_SIZE * gradient
        image = jnp.dot(current.astype(jnp.bfloat16), kept[t], preferred_element_type=jnp.float32)
        residual = measured - lax.psum(image.astype(jnp.bfloat16), "col").astype(jnp.float32)
    gradient = lax.psum_scatter(
        jnp.dot(half, matrix, preferred_element_type=jnp.float32).astype(jnp.bfloat16),
        "row", scatter_dimension=0, tiled=True,
    ).astype(jnp.float32)
    mine = lax.dynamic_slice_in_dim(current, lax.axis_index("row") * rows_mine, rows_mine, 0)
    stepped = jnp.dot(mine, onehot[-2].astype(jnp.float32), precision=HI) + STEP_SIZE * gradient
    keep = jnp.sum(onehot[-1].astype(jnp.float32), axis=0)
    sums = jnp.concatenate([jnp.sum(stepped * stepped, axis=0), jnp.stack(energies)])
    sums = lax.psum(sums, "row")
    return (stepped * keep[None, :], jnp.sqrt(sums[:columns]), sums[columns:] / total_count)


def solution(mesh):
    placed = (P("row", "col"), P(None, "row"), P())
    return jax.shard_map(
        local,
        mesh=mesh,
        in_specs=placed,
        out_specs=(P("row", "col"), P("col"), P()),
        check_vma=False,
    )
```

```python
import functools

import jax
import jax.numpy as jnp
from jax import lax
from jax.experimental import pallas as pl
from jax.experimental.pallas import tpu as pltpu
from jax.sharding import PartitionSpec as P

KMAX = 128
STEP_SIZE = 0.25
LANES = 128
NT = (((1,), (1,)), ((), ()))
F32, BF16 = jnp.float32, jnp.bfloat16
MESH = pl.DeviceIdType.MESH


def dot(a, b):
    return jnp.dot(a, b, preferred_element_type=F32)


def dot_nt(a, b):
    return lax.dot_general(a, b, NT, preferred_element_type=F32)


def pick(values, onehot):
    high = values.astype(BF16)
    rest = values - high.astype(F32)
    mid = rest.astype(BF16)
    low = (rest - mid.astype(F32)).astype(BF16)
    return dot(high, onehot) + dot(mid, onehot) + dot(low, onehot)


def iota(shape, axis):
    return lax.broadcasted_iota(jnp.int32, shape, axis).astype(F32)


def kernel(n_row, n_col, mat, meas, sup, est, norms, energy,
           kept, g0_send, g0_recv, yshard, big, pfull, pair_in, rs_out, rs_in,
           rall, rrows, en_out, en_in, fin_out, fin_in,
           kept_s, kept_r, g0_s, g0_r, y_s, y_r, big_s, big_r, loc,
           pair_s, pair_r, rs_s, rs_r, ag_s, ag_r, rel_s, rel_r, rx_s, rx_r,
           en_s, en_r, fin_s, fin_r):
    r, c = lax.axis_index("row"), lax.axis_index("col")
    n_chip = n_col // 2
    q, h = lax.rem(c, 2), lax.div(c, 2)
    mate = h * 2 + (1 - q)
    mb, width = mat.shape
    signals = meas.shape[0]
    iters, total_k = sup.shape
    ls = signals // n_row
    lh = ls // 2
    msh = mb * n_row // n_chip
    wq = width // n_row
    per = mb // msh

    def remote(src, dst, s, d, row=None, col=None):
        return pltpu.make_async_remote_copy(
            src_ref=src, dst_ref=dst, send_sem=s, recv_sem=d,
            device_id=(r if row is None else row, c if col is None else col),
            device_id_type=MESH)

    barrier = pltpu.get_barrier_semaphore()
    for p in range(1, n_row):
        pl.semaphore_signal(barrier, inc=1, device_id=(lax.rem(r + p, n_row), c), device_id_type=MESH)
    for p in range(1, n_col):
        pl.semaphore_signal(barrier, inc=1, device_id=(r, lax.rem(c + p, n_col)), device_id_type=MESH)

    own_big = pltpu.make_async_copy(mat.at[:, pl.ds(pl.multiple_of(r * wq, LANES), wq)], big.at[r], loc)
    own_big.start()

    offset = (c * width).astype(F32)
    eye = iota((KMAX, KMAX), 0) == iota((KMAX, KMAX), 1)
    index = []
    for t in range(iters):
        local = sup[t:t + 1, :].astype(F32) - offset
        below = jnp.sum(jnp.where(local < 0, 1.0, 0.0), axis=1, keepdims=True)
        slot = iota((1, total_k), 1) - below
        slot = jnp.where((local >= 0) & (local < width), slot, -1.0)
        hit = slot == iota((KMAX, total_k), 0)
        index.append(jnp.max(jnp.where(hit, local, -1.0), axis=1, keepdims=True))

    def onehot(t):
        return jnp.where(index[t] == iota((KMAX, width), 1), 1.0, 0.0).astype(BF16)

    def carried(values, t):
        as_row = jnp.sum(jnp.where(eye, index[t + 1], 0.0), axis=0, keepdims=True)
        same = jnp.where((index[t] == as_row) & (as_row >= 0), 1.0, 0.0).astype(BF16)
        return pick(values, same)

    copies = []

    def gather_kept(t):
        kept[t, r] = dot_nt(onehot(t), mat[...]).astype(BF16)

    def send_kept(t):
        out = []
        for p in range(1, n_row):
            k = remote(kept.at[t, r], kept.at[t, r], kept_s.at[t, p - 1], kept_r.at[t, p - 1],
                       row=lax.rem(r + p, n_row))
            k.start()
            out.append(k)
        return out

    gather_kept(0)
    part = dot_nt(meas[...].astype(BF16), kept[0, r])
    for rr in range(n_row):
        g0_send[rr] = part[rr * ls:(rr + 1) * ls].astype(BF16)
    energy0 = jnp.sum(jnp.sum(meas[...] * meas[...], axis=1, keepdims=True), axis=0, keepdims=True)

    pl.semaphore_wait(barrier, n_row + n_col - 2)

    g0 = []
    for p in range(1, n_row):
        rr = lax.rem(r + p, n_row)
        k = remote(g0_send.at[rr], g0_recv.at[p - 1], g0_s.at[p - 1], g0_r.at[p - 1], row=rr)
        k.start()
        g0.append(k)
    kept_copies = [send_kept(0)]
    holder = lax.div(h * msh, mb)
    yoff = pl.multiple_of(lax.rem(h * msh, mb), LANES)

    def y_copy(p):
        rr = lax.rem(r + p, n_row)
        rows = pl.ds(pl.multiple_of(rr * ls + q * lh, 8), lh)
        return remote(meas.at[rows, pl.ds(yoff, msh)], yshard, y_s.at[p - 1], y_r, row=rr)

    @pl.when(r == holder)
    def _():
        for p in range(1, n_row):
            y_copy(p).start()
        yshard[...] = meas[pl.ds(pl.multiple_of(r * ls + q * lh, 8), lh), pl.ds(yoff, msh)]

    for t in range(1, iters):
        gather_kept(t)
        kept_copies.append(send_kept(t))
    own_big.wait()
    for p in range(1, n_row):
        rr = lax.rem(r + p, n_row)
        k = remote(mat.at[:, pl.ds(pl.multiple_of(rr * wq, LANES), wq)], big.at[r],
                   big_s.at[p - 1], big_r.at[p - 1], row=rr)
        k.start()
        copies.append(k)

    gradient = g0_send[r].astype(F32)
    for k in g0:
        k.wait_recv()
    for p in range(1, n_row):
        gradient = gradient + g0_recv[p - 1].astype(F32)
    current = STEP_SIZE * gradient

    lane = iota((1, LANES), 1)
    shares = jnp.zeros((1, LANES), F32)
    for t in range(iters - 1):
        for k in kept_copies[0] if t == 0 else []:
            k.wait_recv()
        half = current.astype(BF16)
        for rr in range(n_row):
            image = dot(half, kept[t, rr]).astype(BF16)
            for j in range(per):
                pfull[t, rr * per + j] = image[:, j * msh:(j + 1) * msh]
        pair = remote(pfull.at[t, :, pl.ds(pl.multiple_of((1 - q) * lh, 16), lh), :], pair_in.at[t],
                      pair_s.at[t], pair_r.at[t], col=mate)
        pair.start()
        copies.append(pair)
        pair.wait_recv()
        both = pfull[t, :, pl.ds(pl.multiple_of(q * lh, 16), lh), :].astype(F32) + pair_in[t].astype(F32)
        rs_out[t] = both.astype(BF16)
        sends = []
        for p in range(1, n_chip):
            hh = lax.rem(h + p, n_chip)
            k = remote(rs_out.at[t, hh], rs_in.at[t, p - 1], rs_s.at[t, p - 1], rs_r.at[t, p - 1],
                       col=hh * 2 + q)
            k.start()
            sends.append(k)
        predicted = rs_out[t, h].astype(F32)
        if t == 0:
            @pl.when(r != holder)
            def _():
                y_copy(1).wait_recv()
        for p in range(1, n_chip):
            sends[p - 1].wait_recv()
            predicted = predicted + rs_in[t, p - 1].astype(F32)
        copies += sends
        residual = yshard[...] - predicted
        share = jnp.sum(jnp.sum(residual * residual, axis=1, keepdims=True), axis=0, keepdims=True)
        shares = shares + jnp.where(lane == t + 1, share, 0.0)
        rall[t, q, h] = residual.astype(BF16)
        sends = []
        for p in range(1, n_chip):
            hh = lax.rem(h + p, n_chip)
            k = remote(rall.at[t, q, h], rall.at[t, q, h], ag_s.at[t, p - 1], ag_r.at[t, p - 1],
                       col=hh * 2 + q)
            k.start()
            sends.append(k)
        if t == iters - 2:
            en_out[...] = shares
            en_in[c] = shares
            en = []
            for p in range(1, n_col):
                k = remote(en_out, en_in.at[c], en_s.at[p - 1], en_r.at[p - 1],
                           col=lax.rem(c + p, n_col))
                k.start()
                en.append(k)
            copies += en
        for k in sends:
            k.wait_recv()
        copies += sends
        relay = remote(rall.at[t, q], rall.at[t, q], rel_s.at[t], rel_r.at[t], col=mate)
        relay.start()
        copies.append(relay)
        relay.wait_recv()
        if t == iters - 2:
            rx = []
            for p in range(1, n_row):
                k = remote(rall.at[t], rrows.at[p - 1], rx_s.at[p - 1], rx_r.at[p - 1],
                           row=lax.rem(r + p, n_row))
                k.start()
                rx.append(k)
            copies += rx
        full = jnp.concatenate(
            [jnp.concatenate([rall[t, a, b] for b in range(n_chip)], axis=1) for a in range(2)], axis=0)

        def kept_gradient(u):
            return dot_nt(full, jnp.concatenate([kept[u, rr] for rr in range(n_row)], axis=1))

        for k in kept_copies[t + 1]:
            k.wait_recv()
        last = current
        current = carried(current, t) + STEP_SIZE * kept_gradient(t + 1)
    stepped = last + STEP_SIZE * kept_gradient(iters - 2)
    fixed = jnp.sum(stepped * stepped, axis=0, keepdims=True)
    est[...] = pick(current, onehot(iters - 1))

    for k in en:
        k.wait_recv()
    shares = en_in[0]
    for p in range(1, n_col):
        shares = shares + en_in[p]
    shares = shares + jnp.where(lane == 0, energy0, 0.0)

    for k in copies[:n_row - 1]:
        k.wait_recv()
    for k in rx:
        k.wait_recv()
    blocks = [full]
    for p in range(1, n_row):
        blocks.append(jnp.concatenate(
            [jnp.concatenate([rrows[p - 1, a, b] for b in range(n_chip)], axis=1) for a in range(2)], axis=0))
    everyone = jnp.concatenate(blocks, axis=0)
    tile = min(wq, 512)
    for j in range(wq // tile):
        total = jnp.zeros((signals, tile), F32)
        for rr in range(n_row):
            total = total + dot(everyone[:, rr * mb:(rr + 1) * mb], big[rr, :, j * tile:(j + 1) * tile])
        total = STEP_SIZE * total
        fin_out[:, j * tile:(j + 1) * tile] = jnp.sum(total * total, axis=0, keepdims=True)
    fin_out[:, wq:wq + LANES] = fixed
    fin_out[:, wq + LANES:] = shares
    fin_in[r] = fin_out[...]
    fin = []
    for p in range(1, n_row):
        k = remote(fin_out, fin_in.at[r], fin_s.at[p - 1], fin_r.at[p - 1], row=lax.rem(r + p, n_row))
        k.start()
        fin.append(k)
    copies += fin
    for k in fin:
        k.wait_recv()
    ends = fin_in[0, :, wq:]
    for rr in range(1, n_row):
        ends = ends + fin_in[rr, :, wq:]
    as_column = jnp.sum(jnp.where(eye, ends[:, :LANES], 0.0), axis=1, keepdims=True)
    energy[...] = ends[:, LANES:] / (signals * mb * n_row)
    for rr in range(n_row):
        here = index[iters - 2] == iota((KMAX, wq), 1) + rr * wq
        fix = jnp.sum(jnp.where(here, as_column, 0.0), axis=0, keepdims=True)
        mask = jnp.sum(jnp.where(here, 1.0, 0.0), axis=0, keepdims=True)
        norms[:, rr * wq:(rr + 1) * wq] = jnp.sqrt(jnp.where(mask > 0, fix, fin_in[rr, :, :wq]))

    for k in copies:
        k.wait_send()
    for k in g0:
        k.wait_send()
    for group in kept_copies:
        for k in group:
            k.wait_send()

    @pl.when(r == holder)
    def _():
        for p in range(1, n_row):
            y_copy(p).wait_send()


def local(n_row, n_col, matrix, measured, support):
    signals, mb = measured.shape
    width = matrix.shape[1]
    iters = support.shape[0]
    n_chip = n_col // 2
    ls = signals // n_row
    lh = ls // 2
    msh = mb * n_row // n_chip
    wq = width // n_row
    steps = iters - 1
    nr = n_row - 1
    vm = lambda shape, kind: pltpu.VMEM(shape, kind)
    dma = lambda *shape: pltpu.SemaphoreType.DMA(shape)
    scratch = [
        vm((iters, n_row, KMAX, mb), BF16),
        vm((n_row, ls, KMAX), BF16),
        vm((nr, ls, KMAX), BF16),
        vm((lh, msh), F32),
        vm((n_row, mb, wq), BF16),
        vm((steps, n_chip, ls, msh), BF16),
        vm((steps, n_chip, lh, msh), BF16),
        vm((steps, n_chip, lh, msh), BF16),
        vm((steps, n_chip - 1, lh, msh), BF16),
        vm((steps, 2, n_chip, lh, msh), BF16),
        vm((nr, 2, n_chip, lh, msh), BF16),
        vm((1, LANES), F32),
        vm((n_col, 1, LANES), F32),
        vm((1, wq + 2 * LANES), F32),
        vm((n_row, 1, wq + 2 * LANES), F32),
        dma(iters, nr), dma(iters, nr), dma(nr), dma(nr), dma(nr), pltpu.SemaphoreType.DMA,
        dma(nr), dma(nr), pltpu.SemaphoreType.DMA,
        dma(steps), dma(steps), dma(steps, n_chip - 1), dma(steps, n_chip - 1),
        dma(steps, n_chip - 1), dma(steps, n_chip - 1), dma(steps), dma(steps),
        dma(nr), dma(nr), dma(n_col - 1), dma(n_col - 1), dma(nr), dma(nr),
    ]
    vmem = pl.BlockSpec(memory_space=pltpu.VMEM)
    est, norms, energy = pl.pallas_call(
        functools.partial(kernel, n_row, n_col),
        out_shape=(
            jax.ShapeDtypeStruct((ls, width), F32),
            jax.ShapeDtypeStruct((1, width), F32),
            jax.ShapeDtypeStruct((1, LANES), F32),
        ),
        in_specs=[vmem] * 3,
        out_specs=(vmem,) * 3,
        scratch_shapes=scratch,
        compiler_params=pltpu.CompilerParams(
            collective_id=0, has_side_effects=True, vmem_limit_bytes=60 * 2**20),
    )(matrix, measured, support)
    return est, norms.reshape(width), energy[0, :iters]


def solution(mesh):
    placed = (P("row", "col"), P(None, "row"), P())
    return jax.shard_map(
        functools.partial(local, mesh.shape["row"], mesh.shape["col"]),
        mesh=mesh,
        in_specs=placed,
        out_specs=(P("row", "col"), P("col"), P()),
        check_vma=False,
    )
```

```python
import functools

import jax
import jax.numpy as jnp
from jax import lax
from jax.experimental import pallas as pl
from jax.experimental.pallas import tpu as pltpu
from jax.sharding import PartitionSpec as P

KMAX = 128
STEP_SIZE = 0.25
LANES = 128
NT = (((1,), (1,)), ((), ()))
F32, BF16 = jnp.float32, jnp.bfloat16
MESH = pl.DeviceIdType.MESH


def dot(a, b):
    return jnp.dot(a, b, preferred_element_type=F32)


def dot_nt(a, b):
    return lax.dot_general(a, b, NT, preferred_element_type=F32)


def pick(values, onehot):
    high = values.astype(BF16)
    rest = values - high.astype(F32)
    mid = rest.astype(BF16)
    low = (rest - mid.astype(F32)).astype(BF16)
    return dot(high, onehot) + dot(mid, onehot) + dot(low, onehot)


def iota(shape, axis):
    return lax.broadcasted_iota(jnp.int32, shape, axis).astype(F32)


def ahead(columns):
    return columns - columns * 5 // 16 // LANES * LANES


def kernel(n_row, n_col, mat, meas, sup, chosen, where_to, norms, energy,
           kept, g0_send, g0_recv, yshard, big, pfull, pair_in, rs_out, rs_in,
           rall, rrows, en_out, en_in, fin_out, fin_in, gsend, grecv,
           kept_s, kept_r, g0_s, g0_r, y_s, y_r, big_s, big_r, loc,
           pair_s, pair_r, rs_s, rs_r, ag_s, ag_r, rel_s, rel_r, rx_s, rx_r,
           en_s, en_r, fin_s, fin_r, grad_s, grad_r):
    r, c = lax.axis_index("row"), lax.axis_index("col")
    n_chip = n_col // 2
    q, h = lax.rem(c, 2), lax.div(c, 2)
    mate = h * 2 + (1 - q)
    mb, width = mat.shape
    signals = meas.shape[0]
    iters, total_k = sup.shape
    ls = signals // n_row
    lh = ls // 2
    msh = mb * n_row // n_chip
    wq = width // n_row
    wp = ahead(wq)
    per = mb // msh

    def remote(src, dst, s, d, row=None, col=None):
        return pltpu.make_async_remote_copy(
            src_ref=src, dst_ref=dst, send_sem=s, recv_sem=d,
            device_id=(r if row is None else row, c if col is None else col),
            device_id_type=MESH)

    barrier = pltpu.get_barrier_semaphore()
    for p in range(1, n_row):
        pl.semaphore_signal(barrier, inc=1, device_id=(lax.rem(r + p, n_row), c), device_id_type=MESH)
    for p in range(1, n_col):
        pl.semaphore_signal(barrier, inc=1, device_id=(r, lax.rem(c + p, n_col)), device_id_type=MESH)

    own_big = pltpu.make_async_copy(mat.at[:, pl.ds(pl.multiple_of(r * wq, LANES), wp)], big.at[r], loc)
    own_big.start()

    offset = (c * width).astype(F32)
    eye = iota((KMAX, KMAX), 0) == iota((KMAX, KMAX), 1)
    index = []
    for t in range(iters):
        local = sup[t:t + 1, :].astype(F32) - offset
        below = jnp.sum(jnp.where(local < 0, 1.0, 0.0), axis=1, keepdims=True)
        slot = iota((1, total_k), 1) - below
        slot = jnp.where((local >= 0) & (local < width), slot, -1.0)
        hit = slot == iota((KMAX, total_k), 0)
        index.append(jnp.max(jnp.where(hit, local, -1.0), axis=1, keepdims=True))

    def onehot(t):
        return jnp.where(index[t] == iota((KMAX, width), 1), 1.0, 0.0).astype(BF16)

    def carried(values, t):
        as_row = jnp.sum(jnp.where(eye, index[t + 1], 0.0), axis=0, keepdims=True)
        same = jnp.where((index[t] == as_row) & (as_row >= 0), 1.0, 0.0).astype(BF16)
        return pick(values, same)

    copies = []

    def gather_kept(t):
        kept[t, r] = dot_nt(onehot(t), mat[...]).astype(BF16)

    def send_kept(t):
        out = []
        for p in range(1, n_row):
            k = remote(kept.at[t, r], kept.at[t, r], kept_s.at[t, p - 1], kept_r.at[t, p - 1],
                       row=lax.rem(r + p, n_row))
            k.start()
            out.append(k)
        return out

    gather_kept(0)
    part = dot_nt(meas[...].astype(BF16), kept[0, r])
    for rr in range(n_row):
        g0_send[rr] = part[rr * ls:(rr + 1) * ls].astype(BF16)
    energy0 = jnp.sum(jnp.sum(meas[...] * meas[...], axis=1, keepdims=True), axis=0, keepdims=True)

    pl.semaphore_wait(barrier, n_row + n_col - 2)

    g0 = []
    for p in range(1, n_row):
        rr = lax.rem(r + p, n_row)
        k = remote(g0_send.at[rr], g0_recv.at[p - 1], g0_s.at[p - 1], g0_r.at[p - 1], row=rr)
        k.start()
        g0.append(k)
    kept_copies = [send_kept(0)]
    holder = lax.div(h * msh, mb)
    yoff = pl.multiple_of(lax.rem(h * msh, mb), LANES)

    def y_copy(p):
        rr = lax.rem(r + p, n_row)
        rows = pl.ds(pl.multiple_of(rr * ls + q * lh, 8), lh)
        return remote(meas.at[rows, pl.ds(yoff, msh)], yshard, y_s.at[p - 1], y_r, row=rr)

    @pl.when(r == holder)
    def _():
        for p in range(1, n_row):
            y_copy(p).start()
        yshard[...] = meas[pl.ds(pl.multiple_of(r * ls + q * lh, 8), lh), pl.ds(yoff, msh)]

    for t in range(1, iters):
        gather_kept(t)
        kept_copies.append(send_kept(t))
    own_big.wait()
    for p in range(1, n_row):
        rr = lax.rem(r + p, n_row)
        k = remote(mat.at[:, pl.ds(pl.multiple_of(rr * wq, LANES), wp)], big.at[r],
                   big_s.at[p - 1], big_r.at[p - 1], row=rr)
        k.start()
        copies.append(k)

    gradient = g0_send[r].astype(F32)
    for k in g0:
        k.wait_recv()
    for p in range(1, n_row):
        gradient = gradient + g0_recv[p - 1].astype(F32)
    current = STEP_SIZE * gradient

    lane = iota((1, LANES), 1)
    far = sorted(range(1, n_chip), key=lambda p: min(p, n_chip - p), reverse=True)
    shares = jnp.zeros((1, LANES), F32)
    for t in range(iters - 1):
        for k in kept_copies[0] if t == 0 else []:
            k.wait_recv()
        half = current.astype(BF16)
        for rr in range(n_row):
            image = dot(half, kept[t, rr]).astype(BF16)
            for j in range(per):
                pfull[t, rr * per + j] = image[:, j * msh:(j + 1) * msh]
        pair = remote(pfull.at[t, :, pl.ds(pl.multiple_of((1 - q) * lh, 16), lh), :], pair_in.at[t],
                      pair_s.at[t], pair_r.at[t], col=mate)
        pair.start()
        copies.append(pair)
        pair.wait_recv()
        both = pfull[t, :, pl.ds(pl.multiple_of(q * lh, 16), lh), :].astype(F32) + pair_in[t].astype(F32)
        rs_out[t] = both.astype(BF16)
        sends = []
        for p in far:
            hh = lax.rem(h + p, n_chip)
            k = remote(rs_out.at[t, hh], rs_in.at[t, p - 1], rs_s.at[t, p - 1], rs_r.at[t, p - 1],
                       col=hh * 2 + q)
            k.start()
            sends.append(k)
        predicted = rs_out[t, h].astype(F32)
        if t == 0:
            @pl.when(r != holder)
            def _():
                y_copy(1).wait_recv()
        for p, k in zip(reversed(far), reversed(sends)):
            k.wait_recv()
            predicted = predicted + rs_in[t, p - 1].astype(F32)
        copies += sends
        residual = yshard[...] - predicted
        share = jnp.sum(jnp.sum(residual * residual, axis=1, keepdims=True), axis=0, keepdims=True)
        shares = shares + jnp.where(lane == t + 1, share, 0.0)
        rall[t, q, h] = residual.astype(BF16)
        sends = []
        for p in far:
            hh = lax.rem(h + p, n_chip)
            k = remote(rall.at[t, q, h], rall.at[t, q, h], ag_s.at[t, p - 1], ag_r.at[t, p - 1],
                       col=hh * 2 + q)
            k.start()
            sends.append(k)
        if t == iters - 2:
            en_out[...] = shares
            en_in[c] = shares
            en = []
            for p in range(1, n_col):
                k = remote(en_out, en_in.at[c], en_s.at[p - 1], en_r.at[p - 1],
                           col=lax.rem(c + p, n_col))
                k.start()
                en.append(k)
            copies += en
        for k in sends:
            k.wait_recv()
        copies += sends
        relay = remote(rall.at[t, q], rall.at[t, q], rel_s.at[t], rel_r.at[t], col=mate)
        relay.start()
        copies.append(relay)
        relay.wait_recv()
        if t == iters - 2:
            rx = []
            for p in range(1, n_row):
                k = remote(rall.at[t], rrows.at[p - 1], rx_s.at[p - 1], rx_r.at[p - 1],
                           row=lax.rem(r + p, n_row))
                k.start()
                rx.append(k)
            copies += rx
        full = jnp.concatenate(
            [jnp.concatenate([rall[t, a, b] for b in range(n_chip)], axis=1) for a in range(2)], axis=0)

        def kept_gradient(u):
            return dot_nt(full, jnp.concatenate([kept[u, rr] for rr in range(n_row)], axis=1))

        for k in kept_copies[t + 1]:
            k.wait_recv()
        last = current
        current = carried(current, t) + STEP_SIZE * kept_gradient(t + 1)
    stepped = last + STEP_SIZE * kept_gradient(iters - 2)
    fixed = jnp.sum(stepped * stepped, axis=0, keepdims=True)
    chosen[...] = current
    where_to[...] = jnp.broadcast_to(index[iters - 1], (KMAX, KMAX))

    def partial_gradients(m, block):
        sig = lax.rem(r - m + n_row, n_row)
        held = jnp.concatenate(
            [jnp.concatenate([block(a, r * per + j) for j in range(per)], axis=1) for a in range(2)], axis=0)
        for rr in range(n_row):
            cols = slice(rr * wq + wp, (rr + 1) * wq)
            gsend[rr, sig] = dot(held, mat[:, cols]).astype(BF16)
        for p in range(1, n_row):
            rr = lax.rem(r + p, n_row)
            k = remote(gsend.at[rr, sig], grecv.at[p - 1, sig], grad_s.at[p - 1, m], grad_r.at[p - 1, m], row=rr)
            k.start()
            grads.append(k)

    grads = []
    partial_gradients(0, lambda a, b: rall[iters - 2, a, b])
    for p in range(1, n_row):
        rx[p - 1].wait_recv()
        partial_gradients(p, lambda a, b: rrows[p - 1, a, b])

    for k in en:
        k.wait_recv()
    shares = en_in[0]
    for p in range(1, n_col):
        shares = shares + en_in[p]
    shares = shares + jnp.where(lane == 0, energy0, 0.0)

    for k in copies[:n_row - 1]:
        k.wait_recv()
    blocks = [full]
    for p in range(1, n_row):
        blocks.append(jnp.concatenate(
            [jnp.concatenate([rrows[p - 1, a, b] for b in range(n_chip)], axis=1) for a in range(2)], axis=0))
    everyone = jnp.concatenate(blocks, axis=0)
    for j in range(0, wp, 512):
        cols = slice(j, min(j + 512, wp))
        total = dot(everyone[:, :mb], big[0, :, cols])
        for rr in range(1, n_row):
            total = total + dot(everyone[:, rr * mb:(rr + 1) * mb], big[rr, :, cols])
        total = STEP_SIZE * total
        fin_out[:, cols] = jnp.sum(total * total, axis=0, keepdims=True)
    for k in grads:
        k.wait_recv()
    copies += grads
    tail = jnp.zeros((1, wq - wp), F32)
    for sig in range(n_row):
        total = gsend[r, sig].astype(F32)
        for p in range(1, n_row):
            total = total + grecv[p - 1, sig].astype(F32)
        total = STEP_SIZE * total
        tail = tail + jnp.sum(total * total, axis=0, keepdims=True)
    fin_out[:, wp:wq] = tail
    fin_out[:, wq:wq + LANES] = fixed
    fin_out[:, wq + LANES:] = shares
    fin_in[r] = fin_out[...]
    fin = []
    for p in range(1, n_row):
        k = remote(fin_out, fin_in.at[r], fin_s.at[p - 1], fin_r.at[p - 1], row=lax.rem(r + p, n_row))
        k.start()
        fin.append(k)
    copies += fin
    for k in fin:
        k.wait_recv()
    ends = fin_in[0, :, wq:]
    for rr in range(1, n_row):
        ends = ends + fin_in[rr, :, wq:]
    as_column = jnp.sum(jnp.where(eye, ends[:, :LANES], 0.0), axis=1, keepdims=True)
    energy[...] = ends[:, LANES:] / (signals * mb * n_row)
    for rr in range(n_row):
        here = index[iters - 2] == iota((KMAX, wq), 1) + rr * wq
        fix = jnp.sum(jnp.where(here, as_column, 0.0), axis=0, keepdims=True)
        mask = jnp.sum(jnp.where(here, 1.0, 0.0), axis=0, keepdims=True)
        norms[:, rr * wq:(rr + 1) * wq] = jnp.sqrt(jnp.where(mask > 0, fix, fin_in[rr, :, :wq]))

    for k in copies:
        k.wait_send()
    for k in g0:
        k.wait_send()
    for group in kept_copies:
        for k in group:
            k.wait_send()

    @pl.when(r == holder)
    def _():
        for p in range(1, n_row):
            y_copy(p).wait_send()


def expand(chosen, where_to, norms, est, flat):
    tile = est.shape[1]
    start = (pl.program_id(0) * tile).astype(F32)
    hit = where_to[:, :1] - start == iota((KMAX, tile), 1)
    est[...] = pick(chosen[...], jnp.where(hit, 1.0, 0.0).astype(BF16))

    @pl.when(pl.program_id(0) == 0)
    def _():
        flat[...] = norms[...].reshape(flat.shape)


def local(n_row, n_col, matrix, measured, support):
    signals, mb = measured.shape
    width = matrix.shape[1]
    iters = support.shape[0]
    n_chip = n_col // 2
    ls = signals // n_row
    lh = ls // 2
    msh = mb * n_row // n_chip
    wq = width // n_row
    wp = ahead(wq)
    steps = iters - 1
    nr = n_row - 1
    vm = lambda shape, kind: pltpu.VMEM(shape, kind)
    dma = lambda *shape: pltpu.SemaphoreType.DMA(shape)
    scratch = [
        vm((iters, n_row, KMAX, mb), BF16),
        vm((n_row, ls, KMAX), BF16),
        vm((nr, ls, KMAX), BF16),
        vm((lh, msh), F32),
        vm((n_row, mb, wp), BF16),
        vm((steps, n_chip, ls, msh), BF16),
        vm((steps, n_chip, lh, msh), BF16),
        vm((steps, n_chip, lh, msh), BF16),
        vm((steps, n_chip - 1, lh, msh), BF16),
        vm((steps, 2, n_chip, lh, msh), BF16),
        vm((nr, 2, n_chip, lh, msh), BF16),
        vm((1, LANES), F32),
        vm((n_col, 1, LANES), F32),
        vm((1, wq + 2 * LANES), F32),
        vm((n_row, 1, wq + 2 * LANES), F32),
        vm((n_row, n_row, ls, wq - wp), BF16),
        vm((nr, n_row, ls, wq - wp), BF16),
        dma(iters, nr), dma(iters, nr), dma(nr), dma(nr), dma(nr), pltpu.SemaphoreType.DMA,
        dma(nr), dma(nr), pltpu.SemaphoreType.DMA,
        dma(steps), dma(steps), dma(steps, n_chip - 1), dma(steps, n_chip - 1),
        dma(steps, n_chip - 1), dma(steps, n_chip - 1), dma(steps), dma(steps),
        dma(nr), dma(nr), dma(n_col - 1), dma(n_col - 1), dma(nr), dma(nr),
        dma(nr, n_row), dma(nr, n_row),
    ]
    vmem = pl.BlockSpec(memory_space=pltpu.VMEM)
    chosen, where_to, norms, energy = pl.pallas_call(
        functools.partial(kernel, n_row, n_col),
        out_shape=(
            jax.ShapeDtypeStruct((ls, KMAX), F32),
            jax.ShapeDtypeStruct((KMAX, KMAX), F32),
            jax.ShapeDtypeStruct((1, width), F32),
            jax.ShapeDtypeStruct((1, LANES), F32),
        ),
        in_specs=[vmem] * 3,
        out_specs=(vmem,) * 4,
        scratch_shapes=scratch,
        compiler_params=pltpu.CompilerParams(
            collective_id=0, has_side_effects=True, vmem_limit_bytes=60 * 2**20),
    )(matrix, measured, support)
    tile = 512
    est, flat = pl.pallas_call(
        expand,
        grid=(width // tile,),
        out_shape=(jax.ShapeDtypeStruct((ls, width), F32), jax.ShapeDtypeStruct((width,), F32)),
        in_specs=[
            pl.BlockSpec((ls, KMAX), lambda j: (0, 0)),
            pl.BlockSpec((KMAX, KMAX), lambda j: (0, 0)),
            pl.BlockSpec((1, width), lambda j: (0, 0)),
        ],
        out_specs=(
            pl.BlockSpec((ls, tile), lambda j: (0, j)),
            pl.BlockSpec((width,), lambda j: (0,)),
        ),
    )(chosen, where_to, norms)
    return est, flat, energy[0, :iters]


def solution(mesh):
    placed = (P("row", "col"), P(None, "row"), P())
    return jax.shard_map(
        functools.partial(local, mesh.shape["row"], mesh.shape["col"]),
        mesh=mesh,
        in_specs=placed,
        out_specs=(P("row", "col"), P("col"), P()),
        check_vma=False,
    )
```

```python
import functools

import jax
import jax.numpy as jnp
from jax import lax
from jax.experimental import pallas as pl
from jax.experimental.pallas import tpu as pltpu
from jax.sharding import PartitionSpec as P

KMAX = 128
STEP_SIZE = 0.25
LANES = 128
NT = (((1,), (1,)), ((), ()))
F32, BF16 = jnp.float32, jnp.bfloat16
MESH = pl.DeviceIdType.MESH


def dot(a, b):
    return jnp.dot(a, b, preferred_element_type=F32)


def dot_nt(a, b):
    return lax.dot_general(a, b, NT, preferred_element_type=F32)


def pick(values, onehot):
    high = values.astype(BF16)
    rest = values - high.astype(F32)
    mid = rest.astype(BF16)
    low = (rest - mid.astype(F32)).astype(BF16)
    return dot(high, onehot) + dot(mid, onehot) + dot(low, onehot)


def iota(shape, axis):
    return lax.broadcasted_iota(jnp.int32, shape, axis).astype(F32)


def ahead(columns):
    return columns - columns * 5 // 16 // LANES * LANES


def kernel(n_row, n_col, mat, meas, sup, chosen, where_to, norms, energy,
           kept, g0_send, g0_recv, yshard, big, pfull, pair_in, rs_out, rs_in,
           rall, rrows, en_out, en_in, fin_out, fin_in, gsend, grecv,
           kept_s, kept_r, g0_s, g0_r, y_s, y_r, big_s, big_r, loc,
           pair_s, pair_r, rs_s, rs_r, ag_s, ag_r, rel_s, rel_r, rx_s, rx_r,
           en_s, en_r, fin_s, fin_r, grad_s, grad_r, mate_s, mate_r):
    r, c = lax.axis_index("row"), lax.axis_index("col")
    n_chip = n_col // 2
    q, h = lax.rem(c, 2), lax.div(c, 2)
    mate = h * 2 + (1 - q)
    mb, width = mat.shape
    signals = meas.shape[0]
    iters, total_k = sup.shape
    ls = signals // n_row
    lh = ls // 2
    msh = mb * n_row // n_chip
    wq = width // n_row
    wp = ahead(wq)
    per = mb // msh

    def remote(src, dst, s, d, row=None, col=None):
        return pltpu.make_async_remote_copy(
            src_ref=src, dst_ref=dst, send_sem=s, recv_sem=d,
            device_id=(r if row is None else row, c if col is None else col),
            device_id_type=MESH)

    barrier = pltpu.get_barrier_semaphore()
    for p in range(1, n_row):
        pl.semaphore_signal(barrier, inc=1, device_id=(lax.rem(r + p, n_row), c), device_id_type=MESH)
    for p in range(1, n_col):
        pl.semaphore_signal(barrier, inc=1, device_id=(r, lax.rem(c + p, n_col)), device_id_type=MESH)

    own_big = pltpu.make_async_copy(mat.at[:, pl.ds(pl.multiple_of(r * wq, LANES), wp)], big.at[r], loc)
    own_big.start()

    offset = (c * width).astype(F32)
    eye = iota((KMAX, KMAX), 0) == iota((KMAX, KMAX), 1)
    index = []
    for t in range(iters):
        local = sup[t:t + 1, :].astype(F32) - offset
        below = jnp.sum(jnp.where(local < 0, 1.0, 0.0), axis=1, keepdims=True)
        slot = iota((1, total_k), 1) - below
        slot = jnp.where((local >= 0) & (local < width), slot, -1.0)
        hit = slot == iota((KMAX, total_k), 0)
        index.append(jnp.max(jnp.where(hit, local, -1.0), axis=1, keepdims=True))

    def onehot(t):
        return jnp.where(index[t] == iota((KMAX, width), 1), 1.0, 0.0).astype(BF16)

    def carried(values, t):
        as_row = jnp.sum(jnp.where(eye, index[t + 1], 0.0), axis=0, keepdims=True)
        same = jnp.where((index[t] == as_row) & (as_row >= 0), 1.0, 0.0).astype(BF16)
        return pick(values, same)

    copies = []

    def gather_kept(t):
        kept[t, r] = dot_nt(onehot(t), mat[...]).astype(BF16)

    def send_kept(t):
        out = []
        for p in range(1, n_row):
            k = remote(kept.at[t, r], kept.at[t, r], kept_s.at[t, p - 1], kept_r.at[t, p - 1],
                       row=lax.rem(r + p, n_row))
            k.start()
            out.append(k)
        return out

    gather_kept(0)
    part = dot_nt(meas[...].astype(BF16), kept[0, r])
    for rr in range(n_row):
        g0_send[rr] = part[rr * ls:(rr + 1) * ls].astype(BF16)
    energy0 = jnp.sum(jnp.sum(meas[...] * meas[...], axis=1, keepdims=True), axis=0, keepdims=True)

    pl.semaphore_wait(barrier, n_row + n_col - 2)

    g0 = []
    for p in range(1, n_row):
        rr = lax.rem(r + p, n_row)
        k = remote(g0_send.at[rr], g0_recv.at[p - 1], g0_s.at[p - 1], g0_r.at[p - 1], row=rr)
        k.start()
        g0.append(k)
    kept_copies = [send_kept(0)]
    holder = lax.div(h * msh, mb)
    yoff = pl.multiple_of(lax.rem(h * msh, mb), LANES)

    def y_copy(p):
        rr = lax.rem(r + p, n_row)
        rows = pl.ds(pl.multiple_of(rr * ls + q * lh, 8), lh)
        return remote(meas.at[rows, pl.ds(yoff, msh)], yshard, y_s.at[p - 1], y_r, row=rr)

    @pl.when(r == holder)
    def _():
        for p in range(1, n_row):
            y_copy(p).start()
        yshard[...] = meas[pl.ds(pl.multiple_of(r * ls + q * lh, 8), lh), pl.ds(yoff, msh)]

    bulk = []

    def send_ahead(piece):
        rows = pl.ds(piece * (mb // iters), mb // iters)
        for p in range(1, n_row):
            rr = lax.rem(r + p, n_row)
            k = remote(mat.at[rows, pl.ds(pl.multiple_of(rr * wq, LANES), wp)], big.at[r, rows],
                       big_s.at[p - 1, piece], big_r.at[p - 1, piece], row=rr)
            k.start()
            bulk.append(k)

    def further(t):
        gather_kept(t)
        kept_copies.append(send_kept(t))
        send_ahead(t)

    send_ahead(0)

    gradient = g0_send[r].astype(F32)
    for k in g0:
        k.wait_recv()
    for p in range(1, n_row):
        gradient = gradient + g0_recv[p - 1].astype(F32)
    current = STEP_SIZE * gradient

    lane = iota((1, LANES), 1)
    far = sorted(range(1, n_chip), key=lambda p: min(p, n_chip - p), reverse=True)
    shares = jnp.zeros((1, LANES), F32)

    def partial_gradients(grads, m, block):
        sig = lax.rem(r - m + n_row, n_row)
        held = jnp.concatenate(
            [jnp.concatenate([block(a, r * per + j) for j in range(per)], axis=1) for a in range(2)], axis=0)
        for rr in range(n_row):
            cols = slice(rr * wq + wp, (rr + 1) * wq)
            gsend[rr, sig] = dot(held, mat[:, cols]).astype(BF16)
        for p in range(1, n_row):
            rr = lax.rem(r + p, n_row)
            k = remote(gsend.at[rr, sig], grecv.at[p - 1, sig], grad_s.at[p - 1, m], grad_r.at[p - 1, m], row=rr)
            k.start()
            grads.append(k)

    for t in range(iters - 1):
        for k in kept_copies[0] if t == 0 else []:
            k.wait_recv()
        half = current.astype(BF16)
        for rr in range(n_row):
            image = dot(half, kept[t, rr]).astype(BF16)
            for j in range(per):
                pfull[t, rr * per + j] = image[:, j * msh:(j + 1) * msh]
        pair = remote(pfull.at[t, :, pl.ds(pl.multiple_of((1 - q) * lh, 16), lh), :], pair_in.at[t],
                      pair_s.at[t], pair_r.at[t], col=mate)
        pair.start()
        copies.append(pair)
        pair.wait_recv()
        both = pfull[t, :, pl.ds(pl.multiple_of(q * lh, 16), lh), :].astype(F32) + pair_in[t].astype(F32)
        rs_out[t] = both.astype(BF16)
        sends = []
        for p in far:
            hh = lax.rem(h + p, n_chip)
            k = remote(rs_out.at[t, hh], rs_in.at[t, p - 1], rs_s.at[t, p - 1], rs_r.at[t, p - 1],
                       col=hh * 2 + q)
            k.start()
            sends.append(k)
        if t == 0:
            further(1)
        predicted = rs_out[t, h].astype(F32)
        if t == 0:
            @pl.when(r != holder)
            def _():
                y_copy(1).wait_recv()
        for p, k in zip(reversed(far), reversed(sends)):
            k.wait_recv()
            predicted = predicted + rs_in[t, p - 1].astype(F32)
        copies += sends
        residual = yshard[...] - predicted
        share = jnp.sum(jnp.sum(residual * residual, axis=1, keepdims=True), axis=0, keepdims=True)
        shares = shares + jnp.where(lane == t + 1, share, 0.0)
        rall[t, q, h] = residual.astype(BF16)
        sends = []
        for p in far:
            hh = lax.rem(h + p, n_chip)
            k = remote(rall.at[t, q, h], rall.at[t, q, h], ag_s.at[t, p - 1], ag_r.at[t, p - 1],
                       col=hh * 2 + q)
            k.start()
            sends.append(k)
        if t == 0:
            for u in range(2, iters):
                further(u)
        if t == iters - 2:
            en_out[...] = shares
            en_in[c] = shares
            en = []
            for p in range(1, n_col):
                k = remote(en_out, en_in.at[c], en_s.at[p - 1], en_r.at[p - 1],
                           col=lax.rem(c + p, n_col))
                k.start()
                en.append(k)
            copies += en
        for k in sends:
            k.wait_recv()
        copies += sends
        if t == iters - 2:
            rx = []
            for p in range(1, n_row):
                k = remote(rall.at[t, q], rrows.at[p - 1, q], rx_s.at[p - 1], rx_r.at[p - 1],
                           row=lax.rem(r + p, n_row))
                k.start()
                rx.append(k)
            copies += rx
        relay = remote(rall.at[t, q], rall.at[t, q], rel_s.at[t], rel_r.at[t], col=mate)
        relay.start()
        copies.append(relay)
        relay.wait_recv()
        if t == iters - 2:
            grads = []
            partial_gradients(grads, 0, lambda a, b: rall[t, a, b])
        full = jnp.concatenate(
            [jnp.concatenate([rall[t, a, b] for b in range(n_chip)], axis=1) for a in range(2)], axis=0)

        def kept_gradient(u):
            return dot_nt(full, jnp.concatenate([kept[u, rr] for rr in range(n_row)], axis=1))

        for k in kept_copies[t + 1]:
            k.wait_recv()
        last = current
        current = carried(current, t) + STEP_SIZE * kept_gradient(t + 1)
    stepped = last + STEP_SIZE * kept_gradient(iters - 2)
    fixed = jnp.sum(stepped * stepped, axis=0, keepdims=True)
    chosen[...] = current
    where_to[...] = jnp.broadcast_to(index[iters - 1], (KMAX, KMAX))

    for p in range(1, n_row):
        rx[p - 1].wait_recv()
        k = remote(rrows.at[p - 1, q], rrows.at[p - 1, q], mate_s.at[p - 1], mate_r.at[p - 1], col=mate)
        k.start()
        copies.append(k)
        k.wait_recv()
        partial_gradients(grads, p, lambda a, b: rrows[p - 1, a, b])

    for k in en:
        k.wait_recv()
    shares = en_in[0]
    for p in range(1, n_col):
        shares = shares + en_in[p]
    shares = shares + jnp.where(lane == 0, energy0, 0.0)

    own_big.wait()
    for k in bulk:
        k.wait_recv()
    copies += bulk
    blocks = [full]
    for p in range(1, n_row):
        blocks.append(jnp.concatenate(
            [jnp.concatenate([rrows[p - 1, a, b] for b in range(n_chip)], axis=1) for a in range(2)], axis=0))
    everyone = jnp.concatenate(blocks, axis=0)
    for j in range(0, wp, 512):
        cols = slice(j, min(j + 512, wp))
        total = dot(everyone[:, :mb], big[0, :, cols])
        for rr in range(1, n_row):
            total = total + dot(everyone[:, rr * mb:(rr + 1) * mb], big[rr, :, cols])
        total = STEP_SIZE * total
        fin_out[:, cols] = jnp.sum(total * total, axis=0, keepdims=True)
    for k in grads:
        k.wait_recv()
    copies += grads
    tail = jnp.zeros((1, wq - wp), F32)
    for sig in range(n_row):
        total = gsend[r, sig].astype(F32)
        for p in range(1, n_row):
            total = total + grecv[p - 1, sig].astype(F32)
        total = STEP_SIZE * total
        tail = tail + jnp.sum(total * total, axis=0, keepdims=True)
    fin_out[:, wp:wq] = tail
    fin_out[:, wq:wq + LANES] = fixed
    fin_out[:, wq + LANES:] = shares
    fin_in[r] = fin_out[...]
    fin = []
    for p in range(1, n_row):
        k = remote(fin_out, fin_in.at[r], fin_s.at[p - 1], fin_r.at[p - 1], row=lax.rem(r + p, n_row))
        k.start()
        fin.append(k)
    copies += fin
    for k in fin:
        k.wait_recv()
    ends = fin_in[0, :, wq:]
    for rr in range(1, n_row):
        ends = ends + fin_in[rr, :, wq:]
    as_column = jnp.sum(jnp.where(eye, ends[:, :LANES], 0.0), axis=1, keepdims=True)
    energy[...] = ends[:, LANES:] / (signals * mb * n_row)
    for rr in range(n_row):
        here = index[iters - 2] == iota((KMAX, wq), 1) + rr * wq
        fix = jnp.sum(jnp.where(here, as_column, 0.0), axis=0, keepdims=True)
        mask = jnp.sum(jnp.where(here, 1.0, 0.0), axis=0, keepdims=True)
        norms[:, rr * wq:(rr + 1) * wq] = jnp.sqrt(jnp.where(mask > 0, fix, fin_in[rr, :, :wq]))

    for k in copies:
        k.wait_send()
    for k in g0:
        k.wait_send()
    for group in kept_copies:
        for k in group:
            k.wait_send()

    @pl.when(r == holder)
    def _():
        for p in range(1, n_row):
            y_copy(p).wait_send()


def expand(chosen, where_to, norms, sums, est, flat, energy):
    tile = est.shape[1]
    start = (pl.program_id(0) * tile).astype(F32)
    hit = where_to[:, :1] - start == iota((KMAX, tile), 1)
    est[...] = pick(chosen[...], jnp.where(hit, 1.0, 0.0).astype(BF16))

    @pl.when(pl.program_id(0) == 0)
    def _():
        flat[...] = norms[...].reshape(flat.shape)
        for i in range(energy.shape[0]):
            energy[i] = sums[0, i]


def local(n_row, n_col, matrix, measured, support):
    signals, mb = measured.shape
    width = matrix.shape[1]
    iters = support.shape[0]
    n_chip = n_col // 2
    ls = signals // n_row
    lh = ls // 2
    msh = mb * n_row // n_chip
    wq = width // n_row
    wp = ahead(wq)
    steps = iters - 1
    nr = n_row - 1
    vm = lambda shape, kind: pltpu.VMEM(shape, kind)
    dma = lambda *shape: pltpu.SemaphoreType.DMA(shape)
    scratch = [
        vm((iters, n_row, KMAX, mb), BF16),
        vm((n_row, ls, KMAX), BF16),
        vm((nr, ls, KMAX), BF16),
        vm((lh, msh), F32),
        vm((n_row, mb, wp), BF16),
        vm((steps, n_chip, ls, msh), BF16),
        vm((steps, n_chip, lh, msh), BF16),
        vm((steps, n_chip, lh, msh), BF16),
        vm((steps, n_chip - 1, lh, msh), BF16),
        vm((steps, 2, n_chip, lh, msh), BF16),
        vm((nr, 2, n_chip, lh, msh), BF16),
        vm((1, LANES), F32),
        vm((n_col, 1, LANES), F32),
        vm((1, wq + 2 * LANES), F32),
        vm((n_row, 1, wq + 2 * LANES), F32),
        vm((n_row, n_row, ls, wq - wp), BF16),
        vm((nr, n_row, ls, wq - wp), BF16),
        dma(iters, nr), dma(iters, nr), dma(nr), dma(nr), dma(nr), pltpu.SemaphoreType.DMA,
        dma(nr, iters), dma(nr, iters), pltpu.SemaphoreType.DMA,
        dma(steps), dma(steps), dma(steps, n_chip - 1), dma(steps, n_chip - 1),
        dma(steps, n_chip - 1), dma(steps, n_chip - 1), dma(steps), dma(steps),
        dma(nr), dma(nr), dma(n_col - 1), dma(n_col - 1), dma(nr), dma(nr),
        dma(nr, n_row), dma(nr, n_row), dma(nr), dma(nr),
    ]
    vmem = pl.BlockSpec(memory_space=pltpu.VMEM)
    chosen, where_to, norms, energy = pl.pallas_call(
        functools.partial(kernel, n_row, n_col),
        out_shape=(
            jax.ShapeDtypeStruct((ls, KMAX), F32),
            jax.ShapeDtypeStruct((KMAX, KMAX), F32),
            jax.ShapeDtypeStruct((1, width), F32),
            jax.ShapeDtypeStruct((1, LANES), F32),
        ),
        in_specs=[vmem] * 3,
        out_specs=(vmem,) * 4,
        scratch_shapes=scratch,
        compiler_params=pltpu.CompilerParams(
            collective_id=0, has_side_effects=True, vmem_limit_bytes=60 * 2**20),
    )(matrix, measured, support)
    tile = 512
    return pl.pallas_call(
        expand,
        grid=(width // tile,),
        out_shape=(jax.ShapeDtypeStruct((ls, width), F32), jax.ShapeDtypeStruct((width,), F32),
                   jax.ShapeDtypeStruct((iters,), F32)),
        in_specs=[
            pl.BlockSpec((ls, KMAX), lambda j: (0, 0)),
            pl.BlockSpec((KMAX, KMAX), lambda j: (0, 0)),
            pl.BlockSpec((1, width), lambda j: (0, 0)),
            pl.BlockSpec(memory_space=pltpu.SMEM),
        ],
        out_specs=(
            pl.BlockSpec((ls, tile), lambda j: (0, j)),
            pl.BlockSpec((width,), lambda j: (0,)),
            pl.BlockSpec(memory_space=pltpu.SMEM),
        ),
    )(chosen, where_to, norms, energy)


def solution(mesh):
    placed = (P("row", "col"), P(None, "row"), P())
    return jax.shard_map(
        functools.partial(local, mesh.shape["row"], mesh.shape["col"]),
        mesh=mesh,
        in_specs=placed,
        out_specs=(P("row", "col"), P("col"), P()),
        check_vma=False,
    )
```
